512 devices in a mesh: row: 32 (over y, x), col: 16 (over z, core).
Axes of the slice: x: 4, y: 8, z: 8, core: 2. Of those that a mesh axis runs over, the one named last changes fastest.
Arguments:
- weights: bfloat16 [8192, 8192], P('row', 'col'), may hold values from 0.0099487305 to 1
- tile_mask: int32 [64, 64], P('row', 'col'), may hold values from 0 to 1, as said below
Outputs:
- flow: float32 [8192, 8192], P('row', 'col')
The draws below stay inside these ranges and needn't reach their ends.
Inputs may be any that keep to these rules, and one draw needn't show every extreme that they name: `tile_mask`: each column of tiles holds exactly 8 ones, the diagonal tile among them.
All inputs are finite; a program needn't handle non-finite values.
Results may differ from the reference program's by a relative error of at most 0.00095.
Values may be sent and summed in bfloat16 or wider, within the bound.
A program may use at most 64 MiB of HBM per device.

```python
import math
import jax
import jax.numpy as jnp
from jax import lax

TILE = 128
KEEP = 8
NODES = 8192
TILES = 64


def draw_tile_mask(key, part):
    noise = jax.random.randint(key, (TILES, TILES), 0, 1 << 20)
    row_index = lax.broadcasted_iota(jnp.int32, (TILES, TILES), 0)
    col_index = lax.broadcasted_iota(jnp.int32, (TILES, TILES), 1)
    scores = noise * TILES + row_index
    scores = jnp.where(row_index == col_index, jnp.int32(1 << 30), scores)
    ordered = jnp.sort(scores, axis=0)
    cutoff = ordered[TILES - KEEP, :]
    return (scores >= cutoff[None, :]).astype(jnp.int32)


def levels(key, dims, shards, least, top_value):
    loudness, own = 1.0, jax.random.fold_in(key, 6)
    for axis_at, blocks in shards:
        steps = jnp.exp(jax.random.uniform(jax.random.fold_in(own, axis_at), (blocks,), jnp.float32, least / len(shards), top_value / len(shards)))
        loudness = loudness * jnp.repeat(steps, dims[axis_at] // blocks).reshape([-1 if axis == axis_at else 1 for axis in range(len(dims))])
    return loudness


def setup_inputs(seed: int = 0) -> dict:
    seeds = jax.random.split(jax.random.key(seed), 3)
    return {
        "weights": jnp.clip(jnp.exp(math.log(1.0) - 4.61031033 * jax.random.uniform(seeds[0], (NODES, NODES), jnp.float32) ** levels(seeds[0], (NODES, NODES), ((0, 32), (1, 16)), -0.2, 0.2)), 0.0099487305, 1.0).astype(jnp.bfloat16),
        "tile_mask": draw_tile_mask(jax.random.fold_in(seeds[2], 71), 0),
    }


def reference(weights, tile_mask):
    spread = jnp.repeat(jnp.repeat(tile_mask, TILE, axis=0), TILE, axis=1).astype(jnp.float32)
    masked = weights.astype(jnp.float32) * spread
    degree = jnp.sum(masked, axis=0)
    markov = (masked / degree[None, :]).astype(jnp.bfloat16)
    expanded = jnp.dot(markov, markov, preferred_element_type=jnp.float32)
    inflated = expanded * expanded
    mass = jnp.sum(inflated, axis=0)
    return inflated / mass[None, :] * NODES
```

```python
import functools
import jax
import jax.numpy as jnp
from jax import lax
from jax.experimental import pallas as pl
from jax.experimental.pallas import tpu as pltpu
from jax.sharding import PartitionSpec as P

MESH = pl.DeviceIdType.MESH
KEEP = 8
CHIPS_X = 4
CORES = 2
SUBLANES, LANES = 8, 128


def kernel(
    size, rows, cols, mask_ref, w_ref, out_ref, scale_ref,
    block, left, stage, cand_out, cand, right, wide, inflated,
    xm, xd, ym, yd, xs, ys, inv, table, slots,
    s_xm, s_xd, s_ym, s_yd, s_xs, s_ys, s_inv, s_stage, s_cand, s_gy,
    s_gxp, s_gxm, s_rel, s_up, s_down, s_pair, s_local,
):
    nx, ny, nz = CHIPS_X, rows // CHIPS_X, cols // CORES
    tr, tc = block.shape[0] // size, block.shape[1] // size
    r, c = lax.axis_index("row"), lax.axis_index("col")
    x, y = lax.rem(r, nx), lax.div(r, nx)
    core, z = lax.rem(c, CORES), lax.div(c, CORES)
    sends = []

    def wrap(a, n):
        return lax.rem(a + n, n)

    def copy(src, dst, sem, out, arrive, row, col):
        return pltpu.make_async_remote_copy(
            src_ref=src, dst_ref=dst, send_sem=sem.at[0, out], recv_sem=sem.at[1, arrive],
            device_id=(row, col), device_id_type=MESH,
        )

    def send(*args):
        made = copy(*args)
        made.start()
        sends.append(made)

    def at_x(k):
        return y * nx + wrap(x + k, nx), c

    def at_y(k):
        return wrap(y + k, ny) * nx + x, c

    def at_col(k):
        return r, wrap(c + k, cols)

    barrier = pltpu.get_barrier_semaphore()
    partners = [at_x(k) for k in range(1, nx)] + [at_y(k) for k in range(1, ny)]
    partners += [at_col(k) for k in range(1, cols)]
    for partner in partners:
        pl.semaphore_signal(barrier, inc=1, device_id=partner, device_id_type=MESH)

    fetch = pltpu.make_async_copy(w_ref, block, s_local.at[0])
    fetch.start()
    lane = lax.broadcasted_iota(jnp.int32, (SUBLANES, LANES), 1)
    line = lax.broadcasted_iota(jnp.int32, (SUBLANES, LANES), 0)
    own_mask = jnp.zeros((SUBLANES, LANES), jnp.int32)
    for i in range(tr):
        for q in range(tc):
            here = jnp.logical_and(lane == r * tr + i, line == q)
            own_mask = jnp.where(here, mask_ref[i, q], own_mask)
    xm[x] = own_mask
    xs[x] = jnp.zeros((SUBLANES, LANES), jnp.float32)
    fetch.wait()
    degree = jnp.zeros((SUBLANES, LANES), jnp.float32)
    for q in range(tc):
        total = jnp.zeros((1, size), jnp.float32)
        for i in range(tr):
            tile = block[i * size : (i + 1) * size, q * size : (q + 1) * size]
            tile = tile.astype(jnp.float32) * mask_ref[i, q].astype(jnp.float32)
            total += jnp.sum(tile, axis=0, keepdims=True)
            left[c * tc + q, i] = tile.astype(jnp.bfloat16)
        degree = jnp.where(line == q, total, degree)
    xd[x] = degree
    pl.semaphore_wait(barrier, len(partners))

    def to_x(buf, sem):
        for k in range(1, nx):
            send(buf.at[x], buf.at[x], sem, k, x, *at_x(k))

    def from_x(buf, sem):
        for k in range(1, nx):
            other = wrap(x + k, nx)
            copy(buf.at[other], buf.at[other], sem, k, other, *at_x(k)).wait_recv()
        return sum(buf[k] for k in range(nx))

    def to_y(buf, sem):
        for k in range(1, ny):
            send(buf.at[y], buf.at[y], sem, k, y, *at_y(k))

    def from_y(buf, sem):
        for k in range(1, ny):
            other = wrap(y + k, ny)
            copy(buf.at[other], buf.at[other], sem, k, other, *at_y(k)).wait_recv()
        return sum(buf[k] for k in range(ny))

    to_x(xm, s_xm)
    to_x(xd, s_xd)
    for k in range(1, nx):
        other = wrap(x + k, nx)
        send(left.at[c * tc + other], stage.at[x], s_stage, k, x, *at_x(k))

    half = tc // 2

    def chunk(zz, cc, h):
        return left.at[pl.ds((zz * CORES + cc) * tc + h * half, half)]

    def ring_send(way, hop, h):
        part = chunk(wrap(z - way * (hop - 1), nz), core, h)
        sem = s_up if way == 1 else s_down
        n = (hop - 1) * 2 + h
        send(part, part, sem, n, n, r, wrap(z + way, nz) * CORES + core)

    def ring_wait(way, hop, h):
        part = chunk(wrap(z - way * hop, nz), core, h)
        sem = s_up if way == 1 else s_down
        n = (hop - 1) * 2 + h
        copy(part, part, sem, n, n, r, wrap(z - way, nz) * CORES + core).wait_recv()

    def hops(way, h):
        return nz // 2 if (way == 1) == (h == 0) else nz // 2 - 1

    def pair_send(away, h):
        part = chunk(wrap(z + away, nz), core, h)
        n = (away % nz) * 2 + h
        send(part, part, s_pair, n, n, r, z * CORES + 1 - core)

    def pair_wait(away, h):
        part = chunk(wrap(z + away, nz), 1 - core, h)
        n = (away % nz) * 2 + h
        copy(part, part, s_pair, n, n, r, z * CORES + 1 - core).wait_recv()

    def ring_pass(hop, h):
        for way in (1, -1):
            if hop <= hops(way, h):
                ring_wait(way, hop, h)
                if hop + 1 <= hops(way, h):
                    ring_send(way, hop + 1, h)
        for way in (1, -1):
            if hop <= hops(way, h):
                pair_send(-way * hop, h)

    for h in (0, 1):
        for way in (1, -1):
            ring_send(way, 1, h)
    for h in (0, 1):
        pair_send(0, h)
    stage[x] = left[c * tc + x]

    ym[y] = from_x(xm, s_xm)
    to_y(ym, s_ym)
    yd[y] = from_x(xd, s_xd)
    to_y(yd, s_yd)
    ring_pass(1, 0)

    marks = from_y(ym, s_ym)
    count = marks
    step = 1
    while step < rows * tr:
        count += jnp.where(lane >= step, pltpu.roll(count, step, 1), 0)
        step *= 2
    before = count - marks
    ids = jnp.zeros((SUBLANES, LANES), jnp.int32)
    for s in range(KEEP):
        hit = jnp.logical_and(marks == 1, before == s)
        ids = jnp.where(lane == s, jnp.sum(jnp.where(hit, lane, 0), axis=1, keepdims=True), ids)
    table[...] = ids
    fetch = pltpu.make_async_copy(table, slots, s_local.at[1])
    fetch.start()
    inverse = 1.0 / jnp.where(line < tc, from_y(yd, s_yd), 1.0)
    for q in range(tc):
        inv[c * tc + q] = inverse[q : q + 1]
    fetch.wait()

    for k in range(1, nx):
        other = wrap(x + k, nx)
        copy(stage.at[other], stage.at[other], s_stage, k, other, *at_x(k)).wait_recv()
    near = sorted(range(ny), key=lambda k: min(k, ny - k))
    for k in near:
        s = wrap(y + k, ny)
        t = jnp.clip(slots[x, s] - y * (nx * tr), 0, nx * tr - 1)
        tile = stage[lax.div(t, tr), lax.rem(t, tr)]
        if k == 0:
            cand[y] = tile
        else:
            cand_out[k] = tile
    for k in near[1:]:
        send(cand_out.at[k], cand.at[y], s_cand, k, y, *at_y(k))
    for k in range(1, cols):
        mine = inv.at[pl.ds(c * tc, tc)]
        send(mine, mine, s_inv, k, c, *at_col(k))

    ring_pass(1, 1)
    ring_pass(2, 0)
    ring_pass(2, 1)

    for k in near[1:]:
        other = wrap(y + k, ny)
        copy(cand.at[other], cand.at[other], s_cand, k, other, *at_y(k)).wait_recv()
    right[x * KEEP + y] = cand[lax.div(slots[x, y], nx * tr)]

    mine = right.at[x * KEEP + y]
    for k in near[1:]:
        send(mine, mine, s_gy, k, y, *at_y(k))

    def to_neighbours(i):
        part = right.at[x * KEEP + wrap(y + near[i], ny)]
        send(part, part, s_gxp, i, i, *at_x(1))
        send(part, part, s_gxm, i, i, *at_x(-1))

    def from_neighbours(i):
        s = wrap(y + near[i], ny)
        below = right.at[wrap(x - 1, nx) * KEEP + s]
        above = right.at[wrap(x + 1, nx) * KEEP + s]
        copy(below, below, s_gxp, i, i, *at_x(-1)).wait_recv()
        copy(above, above, s_gxm, i, i, *at_x(1)).wait_recv()
        if i % 2 == 0:
            send(below, below, s_rel, i, i, *at_x(1))
        else:
            send(above, above, s_rel, i, i, *at_x(-1))

    to_neighbours(0)
    ring_pass(3, 0)
    for i in range(1, ny):
        k = near[i]
        other = wrap(y + k, ny)
        part = right.at[x * KEEP + other]
        copy(part, part, s_gy, k, other, *at_y(k)).wait_recv()
        to_neighbours(i)
        if i >= 3:
            from_neighbours(i - 3)
        if i == 3:
            ring_pass(3, 1)
    for i in range(ny - 3, ny):
        from_neighbours(i)

    for hop in range(4, nz // 2 + 1):
        for h in (0, 1):
            ring_pass(hop, h)
    for away in range(nz):
        for h in (0, 1):
            pair_wait(away, h)
    for k in range(1, cols):
        other = wrap(c + k, cols)
        part = inv.at[pl.ds(other * tc, tc)]
        copy(part, part, s_inv, k, other, *at_col(k)).wait_recv()
    for q in range(tc):
        for s in range(KEEP):
            tile_row = slots[q, s]
            panel = left[tile_row].reshape(tr * size, size).astype(jnp.float32)
            wide[q, :, s * size : (s + 1) * size] = (panel * inv[tile_row]).astype(jnp.bfloat16)

    for i in range(ny):
        part = right.at[wrap(x + 2, nx) * KEEP + wrap(y + near[i], ny)]
        copy(part, part, s_rel, i, i, *at_x(-1 if i % 2 == 0 else 1)).wait_recv()

    mass = jnp.zeros((SUBLANES, LANES), jnp.float32)
    for q in range(tc):
        tiles = right[q * KEEP : (q + 1) * KEEP].reshape(KEEP * size, size)
        expanded = jnp.dot(wide[q], tiles, preferred_element_type=jnp.float32)
        expanded = expanded * inv[c * tc + q]
        square = expanded * expanded
        inflated[:, q * size : (q + 1) * size] = square
        mass = jnp.where(line == q, jnp.sum(square, axis=0, keepdims=True), mass)
    xs[x] = mass
    to_x(xs, s_xs)
    store = pltpu.make_async_copy(inflated, out_ref, s_local.at[2])
    store.start()
    ys[y] = from_x(xs, s_xs)
    to_y(ys, s_ys)
    nodes = rows * tr * size
    share = nodes / jnp.where(line < tc, from_y(ys, s_ys), 1.0)
    for q in range(tc):
        scale_ref[:, q * size : (q + 1) * size] = share[q : q + 1]
    store.wait()
    for made in sends:
        made.wait_send()


def on_device(weights, tile_mask):
    rows, cols = lax.axis_size("row"), lax.axis_size("col")
    tr, tc = tile_mask.shape
    height, width = weights.shape
    size = height // tr
    nx, ny, nz = CHIPS_X, rows // CHIPS_X, cols // CORES
    tiles = tc * cols
    f32, bf16, i32 = jnp.float32, jnp.bfloat16, jnp.int32
    vmem = pltpu.VMEM
    small = (SUBLANES, LANES)

    def pairs(n):
        return pltpu.SemaphoreType.DMA((2, n))

    inflated, scale = pl.pallas_call(
        functools.partial(kernel, size, rows, cols),
        out_shape=(
            jax.ShapeDtypeStruct((height, width), f32),
            jax.ShapeDtypeStruct((1, width), f32),
        ),
        in_specs=[
            pl.BlockSpec(memory_space=pltpu.SMEM),
            pl.BlockSpec(memory_space=pl.ANY),
        ],
        out_specs=(
            pl.BlockSpec(memory_space=pl.ANY),
            pl.BlockSpec(memory_space=vmem),
        ),
        scratch_shapes=[
            vmem((height, width), bf16),
            vmem((tiles, tr, size, size), bf16),
            vmem((nx, tr, size, size), bf16),
            vmem((ny, size, size), bf16),
            vmem((ny, size, size), bf16),
            vmem((tc * KEEP, size, size), bf16),
            vmem((tc, height, KEEP * size), bf16),
            vmem((height, width), f32),
            vmem((nx, *small), i32),
            vmem((nx, *small), f32),
            vmem((ny, *small), i32),
            vmem((ny, *small), f32),
            vmem((nx, *small), f32),
            vmem((ny, *small), f32),
            vmem((tiles, 1, size), f32),
            vmem(small, i32),
            pltpu.SMEM(small, i32),
            pairs(nx), pairs(nx), pairs(ny), pairs(ny), pairs(nx), pairs(ny),
            pairs(cols), pairs(nx), pairs(ny), pairs(ny),
            pairs(ny), pairs(ny), pairs(ny), pairs(nz), pairs(nz), pairs(2 * nz),
            pltpu.SemaphoreType.DMA((3,)),
        ],
        compiler_params=pltpu.CompilerParams(
            collective_id=0, has_side_effects=True, vmem_limit_bytes=32 * 1024 * 1024
        ),
        name="expand",
    )(tile_mask, weights)
    return inflated * scale


def solution(mesh):
    placed = (P("row", "col"), P("row", "col"))
    return jax.shard_map(
        on_device, mesh=mesh, in_specs=placed, out_specs=P("row", "col"), check_vma=False
    )
```

```python
import functools
import jax
import jax.numpy as jnp
from jax import lax
from jax.experimental import pallas as pl
from jax.experimental.pallas import tpu as pltpu
from jax.sharding import PartitionSpec as P

MESH = pl.DeviceIdType.MESH
KEEP = 8
CHIPS_X = 4
CORES = 2
SUBLANES, LANES = 8, 128


def kernel(
    size, rows, cols, mask_hbm, w_hbm, out_ref, scale_ref,
    mask_ref, block, left, stage, cand_out, cand, right, wide,
    xm, xd, ym, yd, xs, ys, inv, table, slots,
    s_xm, s_xd, s_ym, s_yd, s_xs, s_ys, s_inv, s_stage, s_cand, s_gy,
    s_gxp, s_gxm, s_rel, s_up, s_down, s_pair, s_local,
):
    nx, ny, nz = CHIPS_X, rows // CHIPS_X, cols // CORES
    tr, tc = block.shape[0] // size, block.shape[1] // size
    r, c = lax.axis_index("row"), lax.axis_index("col")
    x, y = lax.rem(r, nx), lax.div(r, nx)
    core, z = lax.rem(c, CORES), lax.div(c, CORES)
    column, h = lax.div(y, tr), lax.rem(y, tr)
    sends = []

    def wrap(a, n):
        return lax.rem(a + n, n)

    def copy(src, dst, sem, out, arrive, row, col):
        return pltpu.make_async_remote_copy(
            src_ref=src, dst_ref=dst, send_sem=sem.at[0, out], recv_sem=sem.at[1, arrive],
            device_id=(row, col), device_id_type=MESH,
        )

    def send(*args):
        made = copy(*args)
        made.start()
        sends.append(made)

    def at_x(k):
        return y * nx + wrap(x + k, nx), c

    def at_y(k):
        return wrap(y + k, ny) * nx + x, c

    def at_col(k):
        return r, wrap(c + k, cols)

    def at_owner(dx, dh):
        return (y - h + wrap(h + dh, tr)) * nx + wrap(x + dx, nx), c

    def slot(xx, yy):
        return lax.div(yy, tr) * KEEP + xx * tr + lax.rem(yy, tr)

    owners = [(dx, dh) for dx in range(nx) for dh in range(tr)]
    near = sorted(range(ny), key=lambda k: min(k, ny - k))
    far = near[:0:-1]

    barrier = pltpu.get_barrier_semaphore()
    partners = [at_x(k) for k in range(1, nx)] + [at_y(k) for k in range(1, ny)]
    partners += [at_col(k) for k in range(1, cols)]
    partners += [at_owner(dx, dh) for dx, dh in owners if dx and dh]
    for partner in partners:
        pl.semaphore_signal(barrier, inc=1, device_id=partner, device_id_type=MESH)

    fetch_mask = pltpu.make_async_copy(mask_hbm, mask_ref, s_local.at[1])
    fetch_mask.start()
    fetch = pltpu.make_async_copy(w_hbm, block, s_local.at[0])
    fetch.start()
    lane = lax.broadcasted_iota(jnp.int32, (SUBLANES, LANES), 1)
    line = lax.broadcasted_iota(jnp.int32, (SUBLANES, LANES), 0)
    xs[x] = jnp.zeros((SUBLANES, LANES), jnp.float32)
    fetch_mask.wait()
    own_mask = jnp.zeros((SUBLANES, LANES), jnp.int32)
    for i in range(tr):
        for q in range(tc):
            here = jnp.logical_and(lane == r * tr + i, line == q)
            own_mask = jnp.where(here, mask_ref[i, q], own_mask)
    ym[y] = own_mask
    fetch.wait()
    degree = jnp.zeros((SUBLANES, LANES), jnp.float32)
    for q in range(tc):
        total = jnp.zeros((1, size), jnp.float32)
        for i in range(tr):
            tile = block[i * size : (i + 1) * size, q * size : (q + 1) * size]
            tile = tile.astype(jnp.float32) * mask_ref[i, q].astype(jnp.float32)
            total += jnp.sum(tile, axis=0, keepdims=True)
            left[c * tc + q, i] = tile.astype(jnp.bfloat16)
        degree = jnp.where(line == q, total, degree)
    yd[y] = degree
    pl.semaphore_wait(barrier, len(partners))

    def to_x(buf, sem):
        for k in range(1, nx):
            send(buf.at[x], buf.at[x], sem, k, x, *at_x(k))

    def from_x(buf, sem):
        for k in range(1, nx):
            other = wrap(x + k, nx)
            copy(buf.at[other], buf.at[other], sem, k, other, *at_x(k)).wait_recv()
        return sum(buf[k] for k in range(nx))

    def to_y(buf, sem):
        for k in far:
            send(buf.at[y], buf.at[y], sem, k, y, *at_y(k))

    def from_y(buf, sem):
        for k in near[1:]:
            other = wrap(y + k, ny)
            copy(buf.at[other], buf.at[other], sem, k, other, *at_y(k)).wait_recv()
        return sum(buf[k] for k in range(ny))

    to_y(ym, s_ym)
    to_y(yd, s_yd)

    def chunk(zz, cc, g):
        return left.at[(zz * CORES + cc) * tc + g]

    def ring_send(way, hop, g):
        part = chunk(wrap(z - way * (hop - 1), nz), core, g)
        sem = s_up if way == 1 else s_down
        n = (hop - 1) * tc + g
        send(part, part, sem, n, n, r, wrap(z + way, nz) * CORES + core)

    def ring_wait(way, hop, g):
        part = chunk(wrap(z - way * hop, nz), core, g)
        sem = s_up if way == 1 else s_down
        n = (hop - 1) * tc + g
        copy(part, part, sem, n, n, r, wrap(z - way, nz) * CORES + core).wait_recv()

    def hops(way, g):
        return nz // 2 if (way == 1) == (g < tc // 2) else nz // 2 - 1

    def pair_send(away, g):
        part = chunk(wrap(z + away, nz), core, g)
        n = (away % nz) * tc + g
        send(part, part, s_pair, n, n, r, z * CORES + 1 - core)

    def pair_wait(away, g):
        part = chunk(wrap(z + away, nz), 1 - core, g)
        n = (away % nz) * tc + g
        copy(part, part, s_pair, n, n, r, z * CORES + 1 - core).wait_recv()

    def turn(way, g):
        return g if way == 1 else (g + tc // 2) % tc

    def ring_pass(hop, g):
        took = [(way, turn(way, g)) for way in (1, -1) if hop <= hops(way, turn(way, g))]
        for way, k in took:
            ring_wait(way, hop, k)
            if hop + 1 <= hops(way, k):
                ring_send(way, hop + 1, k)
        for way, k in took:
            pair_send(-way * hop, k)

    for g in range(tc):
        for way in (1, -1):
            ring_send(way, 1, turn(way, g))
    for k in far:
        other = wrap(y + k, ny)
        part = left.at[c * tc + lax.div(other, tr), lax.rem(other, tr)]
        send(part, stage.at[y], s_stage, k, y, *at_y(k))
    for g in range(tc):
        pair_send(0, g)
    stage[y] = left[c * tc + column, h]

    xm[x] = from_y(ym, s_ym)
    to_x(xm, s_xm)
    xd[x] = from_y(yd, s_yd)
    to_x(xd, s_xd)
    for g in range(tc - 1):
        ring_pass(1, g)

    marks = from_x(xm, s_xm)
    count = marks
    step = 1
    while step < rows * tr:
        count += jnp.where(lane >= step, pltpu.roll(count, step, 1), 0)
        step *= 2
    before = count - marks
    ids = jnp.zeros((SUBLANES, LANES), jnp.int32)
    for s in range(KEEP):
        hit = jnp.logical_and(marks == 1, before == s)
        ids = jnp.where(lane == s, jnp.sum(jnp.where(hit, lane, 0), axis=1, keepdims=True), ids)
    table[...] = ids
    fetch = pltpu.make_async_copy(table, slots, s_local.at[1])
    fetch.start()
    inverse = 1.0 / jnp.where(line < tc, from_x(xd, s_xd), 1.0)
    for q in range(tc):
        inv[c * tc + q] = inverse[q : q + 1]
    for k in near[1:]:
        other = wrap(y + k, ny)
        copy(stage.at[other], stage.at[other], s_stage, k, other, *at_y(k)).wait_recv()
    fetch.wait()

    me = x * tr + h
    for n, (dx, dh) in enumerate(owners):
        s = wrap(x + dx, nx) * tr + wrap(h + dh, tr)
        tile = stage[lax.div(slots[column, s], nx * tr)]
        if n == 0:
            cand[me] = tile
        else:
            cand_out[n] = tile
    order = sorted(range(1, len(owners)), key=lambda n: -min(owners[n][0], nx - owners[n][0]))
    for n in order:
        send(cand_out.at[n], cand.at[me], s_cand, n, me, *at_owner(*owners[n]))
    for k in range(1, cols):
        mine = inv.at[pl.ds(c * tc, tc)]
        send(mine, mine, s_inv, k, c, *at_col(k))

    ring_pass(1, tc - 1)
    for g in range(tc):
        ring_pass(2, g)

    for n in order:
        dx, dh = owners[n]
        other = wrap(x + dx, nx) * tr + wrap(h + dh, tr)
        copy(cand.at[other], cand.at[other], s_cand, n, other, *at_owner(dx, dh)).wait_recv()
    right[slot(x, y)] = cand[lax.rem(slots[column, me], nx * tr)]

    mine = right.at[slot(x, y)]
    for k in near[1:]:
        send(mine, mine, s_gy, k, y, *at_y(k))

    def to_neighbours(i):
        part = right.at[slot(x, wrap(y + near[i], ny))]
        send(part, part, s_gxp, i, i, *at_x(1))
        send(part, part, s_gxm, i, i, *at_x(-1))

    def from_neighbours(i):
        other = wrap(y + near[i], ny)
        below = right.at[slot(wrap(x - 1, nx), other)]
        above = right.at[slot(wrap(x + 1, nx), other)]
        copy(below, below, s_gxp, i, i, *at_x(-1)).wait_recv()
        copy(above, above, s_gxm, i, i, *at_x(1)).wait_recv()
        if i % 2 == 0:
            send(below, below, s_rel, i, i, *at_x(1))
        else:
            send(above, above, s_rel, i, i, *at_x(-1))

    to_neighbours(0)
    ring_pass(3, 0)
    ring_pass(3, 1)
    for i in range(1, ny):
        k = near[i]
        other = wrap(y + k, ny)
        part = right.at[slot(x, other)]
        copy(part, part, s_gy, k, other, *at_y(k)).wait_recv()
        to_neighbours(i)
        if i >= 3:
            from_neighbours(i - 3)
        if i in (2, 3):
            ring_pass(3, i)
    for i in range(ny - 3, ny):
        from_neighbours(i)

    for hop in range(4, nz // 2 + 1):
        for g in range(tc):
            ring_pass(hop, g)
    for away in range(nz):
        for g in range(tc):
            pair_wait(away, g)
    for k in range(1, cols):
        other = wrap(c + k, cols)
        part = inv.at[pl.ds(other * tc, tc)]
        copy(part, part, s_inv, k, other, *at_col(k)).wait_recv()
    for q in range(tc):
        for s in range(KEEP):
            tile_row = slots[q, s]
            panel = left[tile_row].reshape(tr * size, size).astype(jnp.float32)
            wide[q, :, s * size : (s + 1) * size] = (panel * inv[tile_row]).astype(jnp.bfloat16)

    for i in range(ny):
        part = right.at[slot(wrap(x + 2, nx), wrap(y + near[i], ny))]
        copy(part, part, s_rel, i, i, *at_x(-1 if i % 2 == 0 else 1)).wait_recv()

    mass = jnp.zeros((SUBLANES, LANES), jnp.float32)
    for q in range(tc):
        tiles = right[q * KEEP : (q + 1) * KEEP].reshape(KEEP * size, size)
        expanded = jnp.dot(wide[q], tiles, preferred_element_type=jnp.float32)
        expanded = expanded * inv[c * tc + q]
        square = expanded * expanded
        out_ref[:, q * size : (q + 1) * size] = square
        mass = jnp.where(line == q, jnp.sum(square, axis=0, keepdims=True), mass)
    xs[x] = mass
    to_x(xs, s_xs)
    ys[y] = from_x(xs, s_xs)
    to_y(ys, s_ys)
    nodes = rows * tr * size
    share = nodes / jnp.where(line < tc, from_y(ys, s_ys), 1.0)
    for q in range(tc):
        scale_ref[:, q * size : (q + 1) * size] = share[q : q + 1]
    for made in sends:
        made.wait_send()


def on_device(weights, tile_mask):
    rows, cols = lax.axis_size("row"), lax.axis_size("col")
    tr, tc = tile_mask.shape
    height, width = weights.shape
    size = height // tr
    nx, ny, nz = CHIPS_X, rows // CHIPS_X, cols // CORES
    tiles = tc * cols
    f32, bf16, i32 = jnp.float32, jnp.bfloat16, jnp.int32
    vmem = pltpu.VMEM
    small = (SUBLANES, LANES)

    def pairs(n):
        return pltpu.SemaphoreType.DMA((2, n))

    inflated, scale = pl.pallas_call(
        functools.partial(kernel, size, rows, cols),
        out_shape=(
            jax.ShapeDtypeStruct((height, width), f32),
            jax.ShapeDtypeStruct((1, width), f32),
        ),
        in_specs=[
            pl.BlockSpec(memory_space=pltpu.HBM),
            pl.BlockSpec(memory_space=pltpu.HBM),
        ],
        out_specs=(
            pl.BlockSpec(memory_space=vmem),
            pl.BlockSpec(memory_space=vmem),
        ),
        scratch_shapes=[
            pltpu.SMEM((tr, tc), i32),
            vmem((height, width), bf16),
            vmem((tiles, tr, size, size), bf16),
            vmem((ny, size, size), bf16),
            vmem((ny, size, size), bf16),
            vmem((ny, size, size), bf16),
            vmem((tc * KEEP, size, size), bf16),
            vmem((tc, height, KEEP * size), bf16),
            vmem((nx, *small), i32),
            vmem((nx, *small), f32),
            vmem((ny, *small), i32),
            vmem((ny, *small), f32),
            vmem((nx, *small), f32),
            vmem((ny, *small), f32),
            vmem((tiles, 1, size), f32),
            vmem(small, i32),
            pltpu.SMEM(small, i32),
            pairs(nx), pairs(nx), pairs(ny), pairs(ny), pairs(nx), pairs(ny),
            pairs(cols), pairs(ny), pairs(KEEP), pairs(ny),
            pairs(ny), pairs(ny), pairs(ny), pairs(tc * nz // 2), pairs(tc * nz // 2),
            pairs(tc * nz),
            pltpu.SemaphoreType.DMA((2,)),
        ],
        compiler_params=pltpu.CompilerParams(
            collective_id=0, has_side_effects=True, vmem_limit_bytes=32 * 1024 * 1024
        ),
        name="expand",
    )(
        pltpu.with_memory_space_constraint(tile_mask, pltpu.HBM),
        pltpu.with_memory_space_constraint(weights, pltpu.HBM),
    )
    return inflated * scale


def solution(mesh):
    placed = (P("row", "col"), P("row", "col"))
    return jax.shard_map(
        on_device, mesh=mesh, in_specs=placed, out_specs=P("row", "col"), check_vma=False
    )
```

```python
import functools
import jax
import jax.numpy as jnp
from jax import lax
from jax.experimental import pallas as pl
from jax.experimental.pallas import tpu as pltpu
from jax.sharding import PartitionSpec as P

MESH = pl.DeviceIdType.MESH
KEEP = 8
CHIPS_X = 4
CORES = 2
SUBLANES, LANES = 8, 128


def kernel(
    size, rows, cols, mask_hbm, w_hbm, out_ref, scale_ref,
    mask_ref, block, left, stage, cand_out, cand, right, wide,
    xm, xd, ym, yd, xs, ys, inv, table, slots,
    s_xm, s_xd, s_ym, s_yd, s_xs, s_ys, s_inv, s_stage, s_cand, s_gy,
    s_gx, s_next, s_up, s_down, s_pair, s_local,
):
    nx, ny, nz = CHIPS_X, rows // CHIPS_X, cols // CORES
    tr, tc = block.shape[0] // size, block.shape[1] // size
    r, c = lax.axis_index("row"), lax.axis_index("col")
    x, y = lax.rem(r, nx), lax.div(r, nx)
    core, z = lax.rem(c, CORES), lax.div(c, CORES)
    column, h = lax.div(y, tr), lax.rem(y, tr)
    sends = []

    def wrap(a, n):
        return lax.rem(a + n, n)

    def copy(src, dst, sem, out, arrive, row, col):
        return pltpu.make_async_remote_copy(
            src_ref=src, dst_ref=dst, send_sem=sem.at[0, out], recv_sem=sem.at[1, arrive],
            device_id=(row, col), device_id_type=MESH,
        )

    def send(*args):
        made = copy(*args)
        made.start()
        sends.append(made)

    def at_x(k):
        return y * nx + wrap(x + k, nx), c

    def at_y(k):
        return wrap(y + k, ny) * nx + x, c

    def at_col(k):
        return r, wrap(c + k, cols)

    def at_owner(dx, dh):
        return (y - h + wrap(h + dh, tr)) * nx + wrap(x + dx, nx), c

    def slot(xx, yy):
        return lax.div(yy, tr) * KEEP + xx * tr + lax.rem(yy, tr)

    owners = [(dx, dh) for dx in range(nx) for dh in range(tr)]
    near = sorted(range(ny), key=lambda k: min(k, ny - k))
    far = near[:0:-1]

    barrier = pltpu.get_barrier_semaphore()
    partners = [at_x(k) for k in range(1, nx)] + [at_y(k) for k in range(1, ny)]
    partners += [at_col(k) for k in range(1, cols)]
    partners += [at_owner(dx, dh) for dx, dh in owners if dx and dh]
    for partner in partners:
        pl.semaphore_signal(barrier, inc=1, device_id=partner, device_id_type=MESH)

    fetch_mask = pltpu.make_async_copy(mask_hbm, mask_ref, s_local.at[1])
    fetch_mask.start()
    fetch = pltpu.make_async_copy(w_hbm, block, s_local.at[0])
    fetch.start()
    lane = lax.broadcasted_iota(jnp.int32, (SUBLANES, LANES), 1)
    line = lax.broadcasted_iota(jnp.int32, (SUBLANES, LANES), 0)
    xs[x] = jnp.zeros((SUBLANES, LANES), jnp.float32)
    fetch_mask.wait()
    own_mask = jnp.zeros((SUBLANES, LANES), jnp.int32)
    for i in range(tr):
        for q in range(tc):
            here = jnp.logical_and(lane == r * tr + i, line == q)
            own_mask = jnp.where(here, mask_ref[i, q], own_mask)
    ym[y] = own_mask
    fetch.wait()
    degree = jnp.zeros((SUBLANES, LANES), jnp.float32)
    for q in range(tc):
        total = jnp.zeros((1, size), jnp.float32)
        for i in range(tr):
            tile = block[i * size : (i + 1) * size, q * size : (q + 1) * size]
            tile = tile.astype(jnp.float32) * mask_ref[i, q].astype(jnp.float32)
            total += jnp.sum(tile, axis=0, keepdims=True)
            left[c * tc + q, i] = tile.astype(jnp.bfloat16)
        degree = jnp.where(line == q, total, degree)
    yd[y] = degree
    pl.semaphore_wait(barrier, len(partners))

    def to_x(buf, sem):
        for k in range(1, nx):
            send(buf.at[x], buf.at[x], sem, k, x, *at_x(k))

    def from_x(buf, sem):
        for k in range(1, nx):
            other = wrap(x + k, nx)
            copy(buf.at[other], buf.at[other], sem, k, other, *at_x(k)).wait_recv()
        return sum(buf[k] for k in range(nx))

    def to_y(buf, sem):
        for k in far:
            send(buf.at[y], buf.at[y], sem, k, y, *at_y(k))

    def from_y(buf, sem):
        for k in near[1:]:
            other = wrap(y + k, ny)
            copy(buf.at[other], buf.at[other], sem, k, other, *at_y(k)).wait_recv()
        return sum(buf[k] for k in range(ny))

    to_y(ym, s_ym)
    to_y(yd, s_yd)

    def chunk(zz, cc, g):
        return left.at[(zz * CORES + cc) * tc + g]

    def ring_send(way, hop, g):
        part = chunk(wrap(z - way * (hop - 1), nz), core, g)
        sem = s_up if way == 1 else s_down
        n = (hop - 1) * tc + g
        send(part, part, sem, n, n, r, wrap(z + way, nz) * CORES + core)

    def ring_wait(way, hop, g):
        part = chunk(wrap(z - way * hop, nz), core, g)
        sem = s_up if way == 1 else s_down
        n = (hop - 1) * tc + g
        copy(part, part, sem, n, n, r, wrap(z - way, nz) * CORES + core).wait_recv()

    def hops(way, g):
        return nz // 2 if (way == 1) == (g < tc // 2) else nz // 2 - 1

    def pair_send(away, g):
        part = chunk(wrap(z + away, nz), core, g)
        n = (away % nz) * tc + g
        send(part, part, s_pair, n, n, r, z * CORES + 1 - core)

    def pair_wait(away, g):
        part = chunk(wrap(z + away, nz), 1 - core, g)
        n = (away % nz) * tc + g
        copy(part, part, s_pair, n, n, r, z * CORES + 1 - core).wait_recv()

    def turn(way, g):
        return g if way == 1 else (g + tc // 2) % tc

    def ring_pass(hop, g):
        took = [(way, turn(way, g)) for way in (1, -1) if hop <= hops(way, turn(way, g))]
        for way, k in took:
            ring_wait(way, hop, k)
            if hop + 1 <= hops(way, k):
                ring_send(way, hop + 1, k)
        for way, k in took:
            pair_send(-way * hop, k)

    for g in range(tc):
        for way in (1, -1):
            ring_send(way, 1, turn(way, g))
    for k in far:
        other = wrap(y + k, ny)
        part = left.at[c * tc + lax.div(other, tr), lax.rem(other, tr)]
        send(part, stage.at[y], s_stage, k, y, *at_y(k))
    for g in range(tc):
        pair_send(0, g)
    stage[y] = left[c * tc + column, h]

    xm[x] = from_y(ym, s_ym)
    to_x(xm, s_xm)
    xd[x] = from_y(yd, s_yd)
    to_x(xd, s_xd)
    for g in range(tc - 1):
        ring_pass(1, g)

    marks = from_x(xm, s_xm)
    count = marks
    step = 1
    while step < rows * tr:
        count += jnp.where(lane >= step, pltpu.roll(count, step, 1), 0)
        step *= 2
    before = count - marks
    ids = jnp.zeros((SUBLANES, LANES), jnp.int32)
    for s in range(KEEP):
        hit = jnp.logical_and(marks == 1, before == s)
        ids = jnp.where(lane == s, jnp.sum(jnp.where(hit, lane, 0), axis=1, keepdims=True), ids)
    table[...] = ids
    fetch = pltpu.make_async_copy(table, slots, s_local.at[1])
    fetch.start()
    inverse = 1.0 / jnp.where(line < tc, from_x(xd, s_xd), 1.0)
    for q in range(tc):
        inv[c * tc + q] = inverse[q : q + 1]
    for k in near[1:]:
        other = wrap(y + k, ny)
        copy(stage.at[other], stage.at[other], s_stage, k, other, *at_y(k)).wait_recv()
    fetch.wait()

    me = x * tr + h
    for n, (dx, dh) in enumerate(owners):
        s = wrap(x + dx, nx) * tr + wrap(h + dh, tr)
        tile = stage[lax.div(slots[column, s], nx * tr)]
        if n == 0:
            cand[me] = tile
        else:
            cand_out[n] = tile
    order = sorted(range(1, len(owners)), key=lambda n: -min(owners[n][0], nx - owners[n][0]))
    for n in order:
        send(cand_out.at[n], cand.at[me], s_cand, n, me, *at_owner(*owners[n]))
    for k in range(1, cols):
        mine = inv.at[pl.ds(c * tc, tc)]
        send(mine, mine, s_inv, k, c, *at_col(k))

    ring_pass(1, tc - 1)
    for g in range(tc - 1):
        ring_pass(2, g)

    for n in order:
        dx, dh = owners[n]
        other = wrap(x + dx, nx) * tr + wrap(h + dh, tr)
        copy(cand.at[other], cand.at[other], s_cand, n, other, *at_owner(dx, dh)).wait_recv()
    right[slot(x, y)] = cand[lax.rem(slots[column, me], nx * tr)]

    beside = (1, ny - 1)
    spread = sorted(near[1:], key=lambda k: (k in beside, min(k, ny - k)))
    mine = right.at[slot(x, y)]

    def to_others(k):
        part = right.at[slot(x, wrap(y + k, ny))]
        for j in (2, 1, 3):
            send(part, part, s_gx, j * ny + k, j * ny + k, *at_x(j))

    def from_others(k):
        for j in range(1, nx):
            part = right.at[slot(wrap(x - j, nx), wrap(y + k, ny))]
            copy(part, part, s_gx, j * ny + k, j * ny + k, *at_x(-j)).wait_recv()

    to_others(0)
    for k in spread:
        send(mine, mine, s_gy, k, y, *at_y(k))
    ring_pass(2, tc - 1)
    ring_pass(3, 0)
    for n, k in enumerate(spread):
        other = wrap(y + k, ny)
        part = right.at[slot(x, other)]
        copy(part, part, s_gy, k, other, *at_y(k)).wait_recv()
        if k not in beside:
            to_others(k)
        if n == 1:
            from_others(0)
            for j in range(1, nx):
                part = right.at[slot(wrap(x - j, nx), y)]
                for way, to in enumerate((1, -1)):
                    send(part, part, s_next, j * 2 + way, j * 2 + way, *at_y(to))
        if n in (0, 2, 4):
            ring_pass(3, n // 2 + 1)

    for hop in range(4, nz // 2 + 1):
        for g in range(tc):
            ring_pass(hop, g)
    for away in range(nz):
        for g in range(tc):
            pair_wait(away, g)
    for k in range(1, cols):
        other = wrap(c + k, cols)
        part = inv.at[pl.ds(other * tc, tc)]
        copy(part, part, s_inv, k, other, *at_col(k)).wait_recv()
    for q in range(tc):
        for s in range(KEEP):
            tile_row = slots[q, s]
            panel = left[tile_row].reshape(tr * size, size).astype(jnp.float32)
            wide[q, :, s * size : (s + 1) * size] = (panel * inv[tile_row]).astype(jnp.bfloat16)

    for k in range(1, nx):
        for way, to in enumerate((1, -1)):
            part = right.at[slot(wrap(x - k, nx), wrap(y - to, ny))]
            copy(part, part, s_next, k * 2 + way, k * 2 + way, *at_y(-to)).wait_recv()
    for k in spread:
        if k not in beside:
            from_others(k)

    mass = jnp.zeros((SUBLANES, LANES), jnp.float32)
    for q in range(tc):
        tiles = right[q * KEEP : (q + 1) * KEEP].reshape(KEEP * size, size)
        expanded = jnp.dot(wide[q], tiles, preferred_element_type=jnp.float32)
        expanded = expanded * inv[c * tc + q]
        square = expanded * expanded
        out_ref[:, q * size : (q + 1) * size] = square
        mass = jnp.where(line == q, jnp.sum(square, axis=0, keepdims=True), mass)
    xs[x] = mass
    to_x(xs, s_xs)
    ys[y] = from_x(xs, s_xs)
    to_y(ys, s_ys)
    nodes = rows * tr * size
    share = nodes / jnp.where(line < tc, from_y(ys, s_ys), 1.0)
    for q in range(tc):
        scale_ref[:, q * size : (q + 1) * size] = share[q : q + 1]
    for made in sends:
        made.wait_send()


def on_device(weights, tile_mask):
    rows, cols = lax.axis_size("row"), lax.axis_size("col")
    tr, tc = tile_mask.shape
    height, width = weights.shape
    size = height // tr
    nx, ny, nz = CHIPS_X, rows // CHIPS_X, cols // CORES
    tiles = tc * cols
    f32, bf16, i32 = jnp.float32, jnp.bfloat16, jnp.int32
    vmem = pltpu.VMEM
    small = (SUBLANES, LANES)

    def pairs(n):
        return pltpu.SemaphoreType.DMA((2, n))

    inflated, scale = pl.pallas_call(
        functools.partial(kernel, size, rows, cols),
        out_shape=(
            jax.ShapeDtypeStruct((height, width), f32),
            jax.ShapeDtypeStruct((1, width), f32),
        ),
        in_specs=[
            pl.BlockSpec(memory_space=pltpu.HBM),
            pl.BlockSpec(memory_space=pltpu.HBM),
        ],
        out_specs=(
            pl.BlockSpec(memory_space=vmem),
            pl.BlockSpec(memory_space=vmem),
        ),
        scratch_shapes=[
            pltpu.SMEM((tr, tc), i32),
            vmem((height, width), bf16),
            vmem((tiles, tr, size, size), bf16),
            vmem((ny, size, size), bf16),
            vmem((ny, size, size), bf16),
            vmem((ny, size, size), bf16),
            vmem((tc * KEEP, size, size), bf16),
            vmem((tc, height, KEEP * size), bf16),
            vmem((nx, *small), i32),
            vmem((nx, *small), f32),
            vmem((ny, *small), i32),
            vmem((ny, *small), f32),
            vmem((nx, *small), f32),
            vmem((ny, *small), f32),
            vmem((tiles, 1, size), f32),
            vmem(small, i32),
            pltpu.SMEM(small, i32),
            pairs(nx), pairs(nx), pairs(ny), pairs(ny), pairs(nx), pairs(ny),
            pairs(cols), pairs(ny), pairs(KEEP), pairs(ny),
            pairs(nx * ny), pairs(2 * nx), pairs(tc * nz // 2), pairs(tc * nz // 2),
            pairs(tc * nz),
            pltpu.SemaphoreType.DMA((2,)),
        ],
        compiler_params=pltpu.CompilerParams(
            collective_id=0, has_side_effects=True, vmem_limit_bytes=32 * 1024 * 1024
        ),
        name="expand",
    )(
        pltpu.with_memory_space_constraint(tile_mask, pltpu.HBM),
        pltpu.with_memory_space_constraint(weights, pltpu.HBM),
    )
    return inflated * scale


def solution(mesh):
    placed = (P("row", "col"), P("row", "col"))
    return jax.shard_map(
        on_device, mesh=mesh, in_specs=placed, out_specs=P("row", "col"), check_vma=False
    )
```

```python
import functools
import jax
import jax.numpy as jnp
from jax import lax
from jax.experimental import pallas as pl
from jax.experimental.pallas import tpu as pltpu
from jax.sharding import PartitionSpec as P

MESH = pl.DeviceIdType.MESH
KEEP = 8
CHIPS_X = 4
CORES = 2
SUBLANES, LANES = 8, 128


def kernel(
    size, rows, cols, mask_hbm, w_hbm, out_ref, scale_ref,
    mask_ref, block, left, stage, cand_out, cand, right, wide,
    xm, xd, ym, yd, rs, inv, table, slots,
    s_xm, s_xd, s_ym, s_yd, s_rs, s_inv, s_stage, s_cand, s_gy,
    s_gx, s_next, s_up, s_down, s_pair, s_local,
):
    nx, ny, nz = CHIPS_X, rows // CHIPS_X, cols // CORES
    tr, tc = block.shape[0] // size, block.shape[1] // size
    r, c = lax.axis_index("row"), lax.axis_index("col")
    x, y = lax.rem(r, nx), lax.div(r, nx)
    core, z = lax.rem(c, CORES), lax.div(c, CORES)
    column, h = lax.div(y, tr), lax.rem(y, tr)
    sends = []

    def wrap(a, n):
        return lax.rem(a + n, n)

    def copy(src, dst, sem, out, arrive, row, col):
        return pltpu.make_async_remote_copy(
            src_ref=src, dst_ref=dst, send_sem=sem.at[0, out], recv_sem=sem.at[1, arrive],
            device_id=(row, col), device_id_type=MESH,
        )

    def send(*args):
        made = copy(*args)
        made.start()
        sends.append(made)

    def at_x(k):
        return y * nx + wrap(x + k, nx), c

    def at_y(k):
        return wrap(y + k, ny) * nx + x, c

    def at_col(k):
        return r, wrap(c + k, cols)

    def at_row(dx, dy):
        return wrap(y + dy, ny) * nx + wrap(x + dx, nx), c

    def at_owner(dx, dh):
        return (y - h + wrap(h + dh, tr)) * nx + wrap(x + dx, nx), c

    def slot(xx, yy):
        return lax.div(yy, tr) * KEEP + xx * tr + lax.rem(yy, tr)

    owners = [(dx, dh) for dx in range(nx) for dh in range(tr)]
    others = [(dx, dy) for dx in range(nx) for dy in range(ny) if dx or dy]
    others.sort(key=lambda o: -min(o[0], nx - o[0]) - min(o[1], ny - o[1]))
    near = sorted(range(ny), key=lambda k: min(k, ny - k))
    far = near[:0:-1]

    barrier = pltpu.get_barrier_semaphore()
    partners = [at_x(k) for k in range(1, nx)] + [at_y(k) for k in range(1, ny)]
    partners += [at_col(k) for k in range(1, cols)]
    partners += [at_owner(dx, dh) for dx, dh in owners if dx and dh]
    for partner in partners:
        pl.semaphore_signal(barrier, inc=1, device_id=partner, device_id_type=MESH)

    fetch_mask = pltpu.make_async_copy(mask_hbm, mask_ref, s_local.at[1])
    fetch_mask.start()
    fetch = pltpu.make_async_copy(w_hbm, block, s_local.at[0])
    fetch.start()
    lane = lax.broadcasted_iota(jnp.int32, (SUBLANES, LANES), 1)
    line = lax.broadcasted_iota(jnp.int32, (SUBLANES, LANES), 0)
    fetch_mask.wait()
    own_mask = jnp.zeros((SUBLANES, LANES), jnp.int32)
    for i in range(tr):
        for q in range(tc):
            here = jnp.logical_and(lane == r * tr + i, line == q)
            own_mask = jnp.where(here, mask_ref[i, q], own_mask)
    ym[y] = own_mask
    fetch.wait()
    degree = jnp.zeros((SUBLANES, LANES), jnp.float32)
    for q in range(tc):
        total = jnp.zeros((1, size), jnp.float32)
        for i in range(tr):
            tile = block[i * size : (i + 1) * size, q * size : (q + 1) * size]
            tile = tile.astype(jnp.float32) * mask_ref[i, q].astype(jnp.float32)
            total += jnp.sum(tile, axis=0, keepdims=True)
            left[c * tc + q, i] = tile.astype(jnp.bfloat16)
        degree = jnp.where(line == q, total, degree)
    yd[y] = degree
    pl.semaphore_wait(barrier, len(partners))

    def to_x(buf, sem):
        for k in range(1, nx):
            send(buf.at[x], buf.at[x], sem, k, x, *at_x(k))

    def from_x(buf, sem):
        for k in range(1, nx):
            other = wrap(x + k, nx)
            copy(buf.at[other], buf.at[other], sem, k, other, *at_x(k)).wait_recv()
        return sum(buf[k] for k in range(nx))

    def to_y(buf, sem):
        for k in far:
            send(buf.at[y], buf.at[y], sem, k, y, *at_y(k))

    def from_y(buf, sem):
        for k in near[1:]:
            other = wrap(y + k, ny)
            copy(buf.at[other], buf.at[other], sem, k, other, *at_y(k)).wait_recv()
        return sum(buf[k] for k in range(ny))

    to_y(ym, s_ym)
    to_y(yd, s_yd)

    def chunk(zz, cc, g):
        return left.at[(zz * CORES + cc) * tc + g]

    def ring_send(way, hop, g):
        part = chunk(wrap(z - way * (hop - 1), nz), core, g)
        sem = s_up if way == 1 else s_down
        n = (hop - 1) * tc + g
        send(part, part, sem, n, n, r, wrap(z + way, nz) * CORES + core)

    def ring_wait(way, hop, g):
        part = chunk(wrap(z - way * hop, nz), core, g)
        sem = s_up if way == 1 else s_down
        n = (hop - 1) * tc + g
        copy(part, part, sem, n, n, r, wrap(z - way, nz) * CORES + core).wait_recv()

    def hops(way, g):
        return nz // 2 if (way == 1) == (g < tc // 2) else nz // 2 - 1

    def pair_send(away, g):
        part = chunk(wrap(z + away, nz), core, g)
        n = (away % nz) * tc + g
        send(part, part, s_pair, n, n, r, z * CORES + 1 - core)

    def pair_wait(away, g):
        part = chunk(wrap(z + away, nz), 1 - core, g)
        n = (away % nz) * tc + g
        copy(part, part, s_pair, n, n, r, z * CORES + 1 - core).wait_recv()

    def turn(way, g):
        return g if way == 1 else (g + tc // 2) % tc

    def ring_pass(hop, g):
        took = [(way, turn(way, g)) for way in (1, -1) if hop <= hops(way, turn(way, g))]
        for way, k in took:
            ring_wait(way, hop, k)
            if hop + 1 <= hops(way, k):
                ring_send(way, hop + 1, k)
        for way, k in took:
            pair_send(-way * hop, k)

    for g in range(tc):
        for way in (1, -1):
            ring_send(way, 1, turn(way, g))
    for k in far:
        other = wrap(y + k, ny)
        part = left.at[c * tc + lax.div(other, tr), lax.rem(other, tr)]
        send(part, stage.at[y], s_stage, k, y, *at_y(k))
    for g in range(tc):
        pair_send(0, g)
    stage[y] = left[c * tc + column, h]

    xm[x] = from_y(ym, s_ym)
    to_x(xm, s_xm)
    xd[x] = from_y(yd, s_yd)
    to_x(xd, s_xd)
    for g in range(tc - 1):
        ring_pass(1, g)

    marks = from_x(xm, s_xm)
    count = marks
    step = 1
    while step < rows * tr:
        count += jnp.where(lane >= step, pltpu.roll(count, step, 1), 0)
        step *= 2
    before = count - marks
    ids = jnp.zeros((SUBLANES, LANES), jnp.int32)
    for s in range(KEEP):
        hit = jnp.logical_and(marks == 1, before == s)
        ids = jnp.where(lane == s, jnp.sum(jnp.where(hit, lane, 0), axis=1, keepdims=True), ids)
    table[...] = ids
    fetch = pltpu.make_async_copy(table, slots, s_local.at[1])
    fetch.start()
    inverse = 1.0 / jnp.where(line < tc, from_x(xd, s_xd), 1.0)
    for q in range(tc):
        inv[c * tc + q] = inverse[q : q + 1]
    for k in near[1:]:
        other = wrap(y + k, ny)
        copy(stage.at[other], stage.at[other], s_stage, k, other, *at_y(k)).wait_recv()
    fetch.wait()

    me = x * tr + h
    for n, (dx, dh) in enumerate(owners):
        s = wrap(x + dx, nx) * tr + wrap(h + dh, tr)
        tile = stage[lax.div(slots[column, s], nx * tr)]
        if n == 0:
            cand[me] = tile
        else:
            cand_out[n] = tile
    order = sorted(range(1, len(owners)), key=lambda n: -min(owners[n][0], nx - owners[n][0]))
    for n in order:
        send(cand_out.at[n], cand.at[me], s_cand, n, me, *at_owner(*owners[n]))
    for k in range(1, cols):
        mine = inv.at[pl.ds(c * tc, tc)]
        send(mine, mine, s_inv, k, c, *at_col(k))

    ring_pass(1, tc - 1)
    for g in range(tc - 1):
        ring_pass(2, g)

    for n in order:
        dx, dh = owners[n]
        other = wrap(x + dx, nx) * tr + wrap(h + dh, tr)
        copy(cand.at[other], cand.at[other], s_cand, n, other, *at_owner(dx, dh)).wait_recv()
    right[slot(x, y)] = cand[lax.rem(slots[column, me], nx * tr)]

    beside = (1, ny - 1)
    spread = sorted(near[1:], key=lambda k: (k in beside, min(k, ny - k)))
    mine = right.at[slot(x, y)]

    def to_others(k):
        part = right.at[slot(x, wrap(y + k, ny))]
        for j in (2, 1, 3):
            send(part, part, s_gx, j * ny + k, j * ny + k, *at_x(j))

    def from_others(k):
        for j in range(1, nx):
            part = right.at[slot(wrap(x - j, nx), wrap(y + k, ny))]
            copy(part, part, s_gx, j * ny + k, j * ny + k, *at_x(-j)).wait_recv()

    to_others(0)
    for k in spread:
        send(mine, mine, s_gy, k, y, *at_y(k))
    ring_pass(2, tc - 1)
    ring_pass(3, 0)
    for n, k in enumerate(spread):
        other = wrap(y + k, ny)
        part = right.at[slot(x, other)]
        copy(part, part, s_gy, k, other, *at_y(k)).wait_recv()
        if k not in beside:
            to_others(k)
        if n == 1:
            from_others(0)
            for j in range(1, nx):
                part = right.at[slot(wrap(x - j, nx), y)]
                for way, to in enumerate((1, -1)):
                    send(part, part, s_next, j * 2 + way, j * 2 + way, *at_y(to))
        if n in (0, 2, 4):
            ring_pass(3, n // 2 + 1)

    for hop in range(4, nz // 2 + 1):
        for g in range(tc):
            ring_pass(hop, g)
    for away in range(nz):
        for g in range(tc):
            pair_wait(away, g)
    for k in range(1, cols):
        other = wrap(c + k, cols)
        part = inv.at[pl.ds(other * tc, tc)]
        copy(part, part, s_inv, k, other, *at_col(k)).wait_recv()
    for q in range(tc):
        for s in range(KEEP):
            tile_row = slots[q, s]
            panel = left[tile_row].reshape(tr * size, size).astype(jnp.float32)
            wide[q, :, s * size : (s + 1) * size] = (panel * inv[tile_row]).astype(jnp.bfloat16)

    for k in range(1, nx):
        for way, to in enumerate((1, -1)):
            part = right.at[slot(wrap(x - k, nx), wrap(y - to, ny))]
            copy(part, part, s_next, k * 2 + way, k * 2 + way, *at_y(-to)).wait_recv()
    for k in spread:
        if k not in beside:
            from_others(k)

    mass = jnp.zeros((SUBLANES, LANES), jnp.float32)
    for q in range(tc):
        tiles = right[q * KEEP : (q + 1) * KEEP].reshape(KEEP * size, size)
        expanded = jnp.dot(wide[q], tiles, preferred_element_type=jnp.float32)
        expanded = expanded * inv[c * tc + q]
        square = expanded * expanded
        out_ref[:, q * size : (q + 1) * size] = square
        mass = jnp.where(line == q, jnp.sum(square, axis=0, keepdims=True), mass)
    rs[r] = mass[:tc]
    for n, (dx, dy) in enumerate(others):
        send(rs.at[r], rs.at[r], s_rs, n, n, *at_row(dx, dy))
    for n, (dx, dy) in enumerate(others):
        other, col = at_row(nx - dx, ny - dy)
        copy(rs.at[other], rs.at[other], s_rs, n, n, other, col).wait_recv()
    nodes = rows * tr * size
    share = nodes / sum(rs[k] for k in range(rows))
    for q in range(tc):
        scale_ref[:, q * size : (q + 1) * size] = share[q : q + 1]
    for made in sends:
        made.wait_send()


def on_device(weights, tile_mask):
    rows, cols = lax.axis_size("row"), lax.axis_size("col")
    tr, tc = tile_mask.shape
    height, width = weights.shape
    size = height // tr
    nx, ny, nz = CHIPS_X, rows // CHIPS_X, cols // CORES
    tiles = tc * cols
    f32, bf16, i32 = jnp.float32, jnp.bfloat16, jnp.int32
    vmem = pltpu.VMEM
    small = (SUBLANES, LANES)

    def pairs(n):
        return pltpu.SemaphoreType.DMA((2, n))

    inflated, scale = pl.pallas_call(
        functools.partial(kernel, size, rows, cols),
        out_shape=(
            jax.ShapeDtypeStruct((height, width), f32),
            jax.ShapeDtypeStruct((1, width), f32),
        ),
        in_specs=[
            pl.BlockSpec(memory_space=pltpu.HBM),
            pl.BlockSpec(memory_space=pltpu.HBM),
        ],
        out_specs=(
            pl.BlockSpec(memory_space=vmem),
            pl.BlockSpec(memory_space=vmem),
        ),
        scratch_shapes=[
            pltpu.SMEM((tr, tc), i32),
            vmem((height, width), bf16),
            vmem((tiles, tr, size, size), bf16),
            vmem((ny, size, size), bf16),
            vmem((ny, size, size), bf16),
            vmem((ny, size, size), bf16),
            vmem((tc * KEEP, size, size), bf16),
            vmem((tc, height, KEEP * size), bf16),
            vmem((nx, *small), i32),
            vmem((nx, *small), f32),
            vmem((ny, *small), i32),
            vmem((ny, *small), f32),
            vmem((rows, tc, size), f32),
            vmem((tiles, 1, size), f32),
            vmem(small, i32),
            pltpu.SMEM(small, i32),
            pairs(nx), pairs(nx), pairs(ny), pairs(ny), pairs(rows),
            pairs(cols), pairs(ny), pairs(KEEP), pairs(ny),
            pairs(nx * ny), pairs(2 * nx), pairs(tc * nz // 2), pairs(tc * nz // 2),
            pairs(tc * nz),
            pltpu.SemaphoreType.DMA((2,)),
        ],
        compiler_params=pltpu.CompilerParams(
            collective_id=0, has_side_effects=True, vmem_limit_bytes=32 * 1024 * 1024
        ),
        name="expand",
    )(
        pltpu.with_memory_space_constraint(tile_mask, pltpu.HBM),
        pltpu.with_memory_space_constraint(weights, pltpu.HBM),
    )
    return inflated * scale


def solution(mesh):
    placed = (P("row", "col"), P("row", "col"))
    return jax.shard_map(
        on_device, mesh=mesh, in_specs=placed, out_specs=P("row", "col"), check_vma=False
    )
```

```python
import functools
import jax
import jax.numpy as jnp
from jax import lax
from jax.experimental import pallas as pl
from jax.experimental.pallas import tpu as pltpu
from jax.sharding import PartitionSpec as P

MESH = pl.DeviceIdType.MESH
KEEP = 8
CHIPS_X = 4
CORES = 2
SUBLANES, LANES = 8, 128


def kernel(
    size, rows, cols, mask_hbm, w_hbm, out_ref, scale_ref,
    mask_ref, block, left, stage, cand_out, cand, right, wide,
    xm, xd, ym, yd, rs, inv, table, slots,
    s_xm, s_xd, s_ym, s_yd, s_rs, s_inv, s_stage, s_cand, s_gy,
    s_gx, s_next, s_up, s_down, s_pair, s_local,
):
    nx, ny, nz = CHIPS_X, rows // CHIPS_X, cols // CORES
    tr, tc = block.shape[0] // size, block.shape[1] // size
    r, c = lax.axis_index("row"), lax.axis_index("col")
    x, y = lax.rem(r, nx), lax.div(r, nx)
    core, z = lax.rem(c, CORES), lax.div(c, CORES)
    column, h = lax.div(y, tr), lax.rem(y, tr)
    sends = []

    def wrap(a, n):
        return lax.rem(a + n, n)

    def copy(src, dst, sem, out, arrive, row, col):
        return pltpu.make_async_remote_copy(
            src_ref=src, dst_ref=dst, send_sem=sem.at[0, out], recv_sem=sem.at[1, arrive],
            device_id=(row, col), device_id_type=MESH,
        )

    def send(*args):
        made = copy(*args)
        made.start()
        sends.append(made)

    def at_x(k):
        return y * nx + wrap(x + k, nx), c

    def at_y(k):
        return wrap(y + k, ny) * nx + x, c

    def at_col(k):
        return r, wrap(c + k, cols)

    def at_row(dx, dy):
        return wrap(y + dy, ny) * nx + wrap(x + dx, nx), c

    def at_owner(dx, dh):
        return (y - h + wrap(h + dh, tr)) * nx + wrap(x + dx, nx), c

    def slot(xx, yy):
        return lax.div(yy, tr) * KEEP + xx * tr + lax.rem(yy, tr)

    owners = [(dx, dh) for dx in range(nx) for dh in range(tr)]
    others = [(dx, dy) for dx in range(nx) for dy in range(ny) if dx or dy]
    others.sort(key=lambda o: -min(o[0], nx - o[0]) - min(o[1], ny - o[1]))
    near = sorted(range(ny), key=lambda k: min(k, ny - k))
    far = near[:0:-1]

    barrier = pltpu.get_barrier_semaphore()
    partners = [at_x(k) for k in range(1, nx)] + [at_y(k) for k in range(1, ny)]
    partners += [at_col(k) for k in range(1, cols)]
    partners += [at_owner(dx, dh) for dx, dh in owners if dx and dh]
    for partner in partners:
        pl.semaphore_signal(barrier, inc=1, device_id=partner, device_id_type=MESH)

    fetch_mask = pltpu.make_async_copy(mask_hbm, mask_ref, s_local.at[1])
    fetch_mask.start()
    fetch = pltpu.make_async_copy(w_hbm, block, s_local.at[0])
    fetch.start()
    lane = lax.broadcasted_iota(jnp.int32, (SUBLANES, LANES), 1)
    line = lax.broadcasted_iota(jnp.int32, (SUBLANES, LANES), 0)
    fetch_mask.wait()
    own_mask = jnp.zeros((SUBLANES, LANES), jnp.int32)
    for i in range(tr):
        for q in range(tc):
            here = jnp.logical_and(lane == r * tr + i, line == q)
            own_mask = jnp.where(here, mask_ref[i, q], own_mask)
    ym[y] = own_mask
    fetch.wait()
    degree = jnp.zeros((SUBLANES, LANES), jnp.float32)
    for q in range(tc):
        total = jnp.zeros((1, size), jnp.float32)
        for i in range(tr):
            tile = block[i * size : (i + 1) * size, q * size : (q + 1) * size]
            tile = tile.astype(jnp.float32) * mask_ref[i, q].astype(jnp.float32)
            total += jnp.sum(tile, axis=0, keepdims=True)
            left[c * tc + q, i] = tile.astype(jnp.bfloat16)
        degree = jnp.where(line == q, total, degree)
    yd[y] = degree
    pl.semaphore_wait(barrier, len(partners))

    def to_x(buf, sem):
        for k in range(1, nx):
            send(buf.at[x], buf.at[x], sem, k, x, *at_x(k))

    def from_x(buf, sem):
        for k in range(1, nx):
            other = wrap(x + k, nx)
            copy(buf.at[other], buf.at[other], sem, k, other, *at_x(k)).wait_recv()
        return sum(buf[k] for k in range(nx))

    def to_y(buf, sem):
        for k in far:
            send(buf.at[y], buf.at[y], sem, k, y, *at_y(k))

    def from_y(buf, sem):
        for k in near[1:]:
            other = wrap(y + k, ny)
            copy(buf.at[other], buf.at[other], sem, k, other, *at_y(k)).wait_recv()
        return sum(buf[k] for k in range(ny))

    to_y(ym, s_ym)
    to_y(yd, s_yd)

    def chunk(zz, cc, g):
        return left.at[(zz * CORES + cc) * tc + g]

    def ring_send(way, hop, g):
        part = chunk(wrap(z - way * (hop - 1), nz), core, g)
        sem = s_up if way == 1 else s_down
        n = (hop - 1) * tc + g
        send(part, part, sem, n, n, r, wrap(z + way, nz) * CORES + core)

    def ring_wait(way, hop, g):
        part = chunk(wrap(z - way * hop, nz), core, g)
        sem = s_up if way == 1 else s_down
        n = (hop - 1) * tc + g
        copy(part, part, sem, n, n, r, wrap(z - way, nz) * CORES + core).wait_recv()

    def hops(way, g):
        return nz // 2 if (way == 1) == (g < tc // 2) else nz // 2 - 1

    def pair_send(away, g):
        part = chunk(wrap(z + away, nz), core, g)
        n = (away % nz) * tc + g
        send(part, part, s_pair, n, n, r, z * CORES + 1 - core)

    def pair_wait(away, g):
        part = chunk(wrap(z + away, nz), 1 - core, g)
        n = (away % nz) * tc + g
        copy(part, part, s_pair, n, n, r, z * CORES + 1 - core).wait_recv()

    def turn(way, g):
        return g if way == 1 else (g + tc // 2) % tc

    def ring_pass(hop, g):
        took = [(way, turn(way, g)) for way in (1, -1) if hop <= hops(way, turn(way, g))]
        for way, k in took:
            ring_wait(way, hop, k)
            if hop + 1 <= hops(way, k):
                ring_send(way, hop + 1, k)
        for way, k in took:
            pair_send(-way * hop, k)

    for g in range(tc):
        for way in (1, -1):
            ring_send(way, 1, turn(way, g))
    for k in far:
        other = wrap(y + k, ny)
        part = left.at[c * tc + lax.div(other, tr), lax.rem(other, tr)]
        send(part, stage.at[y], s_stage, k, y, *at_y(k))
    for g in range(tc):
        pair_send(0, g)
    stage[y] = left[c * tc + column, h]

    xm[x] = from_y(ym, s_ym)
    to_x(xm, s_xm)
    xd[x] = from_y(yd, s_yd)
    to_x(xd, s_xd)
    for g in range(tc - 1):
        ring_pass(1, g)

    marks = from_x(xm, s_xm)
    count = marks
    step = 1
    while step < rows * tr:
        count += jnp.where(lane >= step, pltpu.roll(count, step, 1), 0)
        step *= 2
    before = count - marks
    ids = jnp.zeros((SUBLANES, LANES), jnp.int32)
    for s in range(KEEP):
        hit = jnp.logical_and(marks == 1, before == s)
        ids = jnp.where(lane == s, jnp.sum(jnp.where(hit, lane, 0), axis=1, keepdims=True), ids)
    table[...] = ids
    fetch = pltpu.make_async_copy(table, slots, s_local.at[1])
    fetch.start()
    inverse = 1.0 / jnp.where(line < tc, from_x(xd, s_xd), 1.0)
    for q in range(tc):
        inv[c * tc + q] = inverse[q : q + 1]
    for k in near[1:]:
        other = wrap(y + k, ny)
        copy(stage.at[other], stage.at[other], s_stage, k, other, *at_y(k)).wait_recv()
    fetch.wait()

    me = x * tr + h
    for n, (dx, dh) in enumerate(owners):
        s = wrap(x + dx, nx) * tr + wrap(h + dh, tr)
        tile = stage[lax.div(slots[column, s], nx * tr)]
        if n == 0:
            cand[me] = tile
        else:
            cand_out[n] = tile
    order = sorted(range(1, len(owners)), key=lambda n: -min(owners[n][0], nx - owners[n][0]))
    for n in order:
        send(cand_out.at[n], cand.at[me], s_cand, n, me, *at_owner(*owners[n]))
    for k in range(1, cols):
        mine = inv.at[pl.ds(c * tc, tc)]
        send(mine, mine, s_inv, k, c, *at_col(k))

    ring_pass(1, tc - 1)
    for g in range(tc - 1):
        ring_pass(2, g)

    for n in order:
        dx, dh = owners[n]
        other = wrap(x + dx, nx) * tr + wrap(h + dh, tr)
        copy(cand.at[other], cand.at[other], s_cand, n, other, *at_owner(dx, dh)).wait_recv()
    right[slot(x, y)] = cand[lax.rem(slots[column, me], nx * tr)]

    beside = (1, ny - 1)
    spread = sorted(near[1:], key=lambda k: (k in beside, min(k, ny - k)))
    mine = right.at[slot(x, y)]

    def to_others(k):
        part = right.at[slot(x, wrap(y + k, ny))]
        for j in (2, 1, 3):
            send(part, part, s_gx, j * ny + k, j * ny + k, *at_x(j))

    def from_others(k):
        for j in range(1, nx):
            part = right.at[slot(wrap(x - j, nx), wrap(y + k, ny))]
            copy(part, part, s_gx, j * ny + k, j * ny + k, *at_x(-j)).wait_recv()

    to_others(0)
    for k in spread:
        send(mine, mine, s_gy, k, y, *at_y(k))
    ring_pass(2, tc - 1)
    ring_pass(3, 0)
    for n, k in enumerate(spread):
        other = wrap(y + k, ny)
        part = right.at[slot(x, other)]
        copy(part, part, s_gy, k, other, *at_y(k)).wait_recv()
        if k not in beside:
            to_others(k)
        if n == 1:
            from_others(0)
            for j in range(1, nx):
                part = right.at[slot(wrap(x - j, nx), y)]
                for way, to in enumerate((1, -1)):
                    send(part, part, s_next, j * 2 + way, j * 2 + way, *at_y(to))
        if n in (0, 2, 4):
            ring_pass(3, n // 2 + 1)

    for hop in range(4, nz // 2 + 1):
        for g in range(tc):
            ring_pass(hop, g)
    for away in range(nz):
        for g in range(tc):
            pair_wait(away, g)
    for k in range(1, cols):
        other = wrap(c + k, cols)
        part = inv.at[pl.ds(other * tc, tc)]
        copy(part, part, s_inv, k, other, *at_col(k)).wait_recv()
    for q in range(tc):
        for s in range(KEEP):
            tile_row = slots[q, s]
            panel = left[tile_row].reshape(tr * size, size).astype(jnp.float32)
            wide[q, :, s * size : (s + 1) * size] = (panel * inv[tile_row]).astype(jnp.bfloat16)

    for k in range(1, nx):
        for way, to in enumerate((1, -1)):
            part = right.at[slot(wrap(x - k, nx), wrap(y - to, ny))]
            copy(part, part, s_next, k * 2 + way, k * 2 + way, *at_y(-to)).wait_recv()
    for k in spread:
        if k not in beside:
            from_others(k)

    mass = jnp.zeros((SUBLANES, LANES), jnp.float32)
    for q in range(tc):
        tiles = right[q * KEEP : (q + 1) * KEEP].reshape(KEEP * size, size)
        expanded = jnp.dot(wide[q], tiles, preferred_element_type=jnp.float32)
        expanded = expanded * inv[c * tc + q]
        square = expanded * expanded
        out_ref[:, q * size : (q + 1) * size] = square
        mass = jnp.where(line == q, jnp.sum(square, axis=0, keepdims=True), mass)
    rs[r] = mass[:tc]
    for n, (dx, dy) in enumerate(others):
        send(rs.at[r], rs.at[r], s_rs, n, n, *at_row(dx, dy))
    for made in sends:
        made.wait_send()
    for n, (dx, dy) in enumerate(others):
        other, col = at_row(nx - dx, ny - dy)
        copy(rs.at[other], rs.at[other], s_rs, n, n, other, col).wait_recv()
    nodes = rows * tr * size
    share = nodes / sum(rs[k] for k in range(rows))
    for q in range(tc):
        scale_ref[:, q * size : (q + 1) * size] = share[q : q + 1]


def on_device(weights, tile_mask):
    rows, cols = lax.axis_size("row"), lax.axis_size("col")
    tr, tc = tile_mask.shape
    height, width = weights.shape
    size = height // tr
    nx, ny, nz = CHIPS_X, rows // CHIPS_X, cols // CORES
    tiles = tc * cols
    f32, bf16, i32 = jnp.float32, jnp.bfloat16, jnp.int32
    vmem = pltpu.VMEM
    small = (SUBLANES, LANES)

    def pairs(n):
        return pltpu.SemaphoreType.DMA((2, n))

    inflated, scale = pl.pallas_call(
        functools.partial(kernel, size, rows, cols),
        out_shape=(
            jax.ShapeDtypeStruct((height, width), f32),
            jax.ShapeDtypeStruct((1, width), f32),
        ),
        in_specs=[
            pl.BlockSpec(memory_space=pltpu.HBM),
            pl.BlockSpec(memory_space=pltpu.HBM),
        ],
        out_specs=(
            pl.BlockSpec(memory_space=vmem),
            pl.BlockSpec(memory_space=vmem),
        ),
        scratch_shapes=[
            pltpu.SMEM((tr, tc), i32),
            vmem((height, width), bf16),
            vmem((tiles, tr, size, size), bf16),
            vmem((ny, size, size), bf16),
            vmem((ny, size, size), bf16),
            vmem((ny, size, size), bf16),
            vmem((tc * KEEP, size, size), bf16),
            vmem((tc, height, KEEP * size), bf16),
            vmem((nx, *small), i32),
            vmem((nx, *small), f32),
            vmem((ny, *small), i32),
            vmem((ny, *small), f32),
            vmem((rows, tc, size), f32),
            vmem((tiles, 1, size), f32),
            vmem(small, i32),
            pltpu.SMEM(small, i32),
            pairs(nx), pairs(nx), pairs(ny), pairs(ny), pairs(rows),
            pairs(cols), pairs(ny), pairs(KEEP), pairs(ny),
            pairs(nx * ny), pairs(2 * nx), pairs(tc * nz // 2), pairs(tc * nz // 2),
            pairs(tc * nz),
            pltpu.SemaphoreType.DMA((2,)),
        ],
        compiler_params=pltpu.CompilerParams(
            collective_id=0, has_side_effects=True, vmem_limit_bytes=32 * 1024 * 1024
        ),
        name="expand",
    )(
        pltpu.with_memory_space_constraint(tile_mask, pltpu.HBM),
        pltpu.with_memory_space_constraint(weights, pltpu.HBM),
    )
    return inflated * scale


def solution(mesh):
    placed = (P("row", "col"), P("row", "col"))
    return jax.shard_map(
        on_device, mesh=mesh, in_specs=placed, out_specs=P("row", "col"), check_vma=False
    )
```

```python
import functools
import jax
import jax.numpy as jnp
from jax import lax
from jax.experimental import pallas as pl
from jax.experimental.pallas import tpu as pltpu
from jax.sharding import PartitionSpec as P

MESH = pl.DeviceIdType.MESH
KEEP = 8
CHIPS_X = 4
CORES = 2
SUBLANES, LANES = 4, 128


def kernel(
    size, rows, cols, mask_hbm, w_hbm, out_ref, scale_ref,
    mask_ref, block, left, stage, cand_out, cand, right, wide,
    xm, xd, ym, yd, rs, inv, table, slots,
    s_xm, s_xd, s_ym, s_yd, s_rs, s_inv, s_stage, s_cand, s_gy,
    s_gx, s_next, s_up, s_down, s_pair, s_local,
):
    nx, ny, nz = CHIPS_X, rows // CHIPS_X, cols // CORES
    tr, tc = block.shape[0] // size, block.shape[1] // size
    r, c = lax.axis_index("row"), lax.axis_index("col")
    x, y = lax.rem(r, nx), lax.div(r, nx)
    core, z = lax.rem(c, CORES), lax.div(c, CORES)
    column, h = lax.div(y, tr), lax.rem(y, tr)
    sends = []

    def wrap(a, n):
        return lax.rem(a + n, n)

    def copy(src, dst, sem, out, arrive, row, col):
        return pltpu.make_async_remote_copy(
            src_ref=src, dst_ref=dst, send_sem=sem.at[0, out], recv_sem=sem.at[1, arrive],
            device_id=(row, col), device_id_type=MESH,
        )

    def send(*args):
        made = copy(*args)
        made.start()
        sends.append(made)

    def at_x(k):
        return y * nx + wrap(x + k, nx), c

    def at_y(k):
        return wrap(y + k, ny) * nx + x, c

    def at_col(k):
        return r, wrap(c + k, cols)

    def at_row(dx, dy):
        return wrap(y + dy, ny) * nx + wrap(x + dx, nx), c

    def at_owner(dx, dh):
        return (y - h + wrap(h + dh, tr)) * nx + wrap(x + dx, nx), c

    def slot(xx, yy):
        return lax.div(yy, tr) * KEEP + xx * tr + lax.rem(yy, tr)

    owners = [(dx, dh) for dx in range(nx) for dh in range(tr)]
    others = [(dx, dy) for dx in range(nx) for dy in range(ny) if dx or dy]
    others.sort(key=lambda o: -min(o[0], nx - o[0]) - min(o[1], ny - o[1]))
    near = sorted(range(ny), key=lambda k: min(k, ny - k))
    far = near[:0:-1]

    barrier = pltpu.get_barrier_semaphore()
    partners = [at_x(k) for k in range(1, nx)] + [at_y(k) for k in range(1, ny)]
    partners += [at_col(k) for k in range(1, cols)]
    partners += [at_owner(dx, dh) for dx, dh in owners if dx and dh]
    for partner in partners:
        pl.semaphore_signal(barrier, inc=1, device_id=partner, device_id_type=MESH)

    fetch_mask = pltpu.make_async_copy(mask_hbm, mask_ref, s_local.at[1])
    fetch_mask.start()
    fetch = pltpu.make_async_copy(w_hbm, block, s_local.at[0])
    fetch.start()
    lane = lax.broadcasted_iota(jnp.int32, (SUBLANES, LANES), 1)
    line = lax.broadcasted_iota(jnp.int32, (SUBLANES, LANES), 0)
    fetch_mask.wait()
    own_mask = jnp.zeros((SUBLANES, LANES), jnp.int32)
    for i in range(tr):
        for q in range(tc):
            here = jnp.logical_and(lane == r * tr + i, line == q)
            own_mask = jnp.where(here, mask_ref[i, q], own_mask)
    ym[y] = own_mask
    fetch.wait()
    degree = jnp.zeros((SUBLANES, LANES), jnp.float32)
    for q in range(tc):
        total = jnp.zeros((1, size), jnp.float32)
        for i in range(tr):
            tile = block[i * size : (i + 1) * size, q * size : (q + 1) * size]
            tile = tile.astype(jnp.float32) * mask_ref[i, q].astype(jnp.float32)
            total += jnp.sum(tile, axis=0, keepdims=True)
            left[c * tc + q, i] = tile.astype(jnp.bfloat16)
        degree = jnp.where(line == q, total, degree)
    yd[y] = degree
    pl.semaphore_wait(barrier, len(partners))

    def to_x(buf, sem):
        for k in range(1, nx):
            send(buf.at[x], buf.at[x], sem, k, x, *at_x(k))

    def from_x(buf, sem):
        for k in range(1, nx):
            other = wrap(x + k, nx)
            copy(buf.at[other], buf.at[other], sem, k, other, *at_x(k)).wait_recv()
        return sum(buf[k] for k in range(nx))

    def to_y(buf, sem):
        for k in far:
            send(buf.at[y], buf.at[y], sem, k, y, *at_y(k))

    def from_y(buf, sem):
        for k in near[1:]:
            other = wrap(y + k, ny)
            copy(buf.at[other], buf.at[other], sem, k, other, *at_y(k)).wait_recv()
        return sum(buf[k] for k in range(ny))

    to_y(ym, s_ym)
    to_y(yd, s_yd)

    def chunk(zz, cc, g):
        return left.at[(zz * CORES + cc) * tc + g]

    def ring_send(way, hop, g):
        part = chunk(wrap(z - way * (hop - 1), nz), core, g)
        sem = s_up if way == 1 else s_down
        n = (hop - 1) * tc + g
        send(part, part, sem, n, n, r, wrap(z + way, nz) * CORES + core)

    def ring_wait(way, hop, g):
        part = chunk(wrap(z - way * hop, nz), core, g)
        sem = s_up if way == 1 else s_down
        n = (hop - 1) * tc + g
        copy(part, part, sem, n, n, r, wrap(z - way, nz) * CORES + core).wait_recv()

    def hops(way, g):
        return nz // 2 if (way == 1) == (g < tc // 2) else nz // 2 - 1

    def pair_send(away, g):
        part = chunk(wrap(z + away, nz), core, g)
        n = (away % nz) * tc + g
        send(part, part, s_pair, n, n, r, z * CORES + 1 - core)

    def pair_wait(away, g):
        part = chunk(wrap(z + away, nz), 1 - core, g)
        n = (away % nz) * tc + g
        copy(part, part, s_pair, n, n, r, z * CORES + 1 - core).wait_recv()

    def turn(way, g):
        return g if way == 1 else (g + tc // 2) % tc

    def ring_pass(hop, g):
        took = [(way, turn(way, g)) for way in (1, -1) if hop <= hops(way, turn(way, g))]
        for way, k in took:
            ring_wait(way, hop, k)
            if hop + 1 <= hops(way, k):
                ring_send(way, hop + 1, k)
        for way, k in took:
            pair_send(-way * hop, k)

    for g in range(tc):
        for way in (1, -1):
            ring_send(way, 1, turn(way, g))
    for k in far:
        other = wrap(y + k, ny)
        part = left.at[c * tc + lax.div(other, tr), lax.rem(other, tr)]
        send(part, stage.at[y], s_stage, k, y, *at_y(k))
    for g in range(tc):
        pair_send(0, g)
    stage[y] = left[c * tc + column, h]

    xm[x] = from_y(ym, s_ym)
    to_x(xm, s_xm)
    xd[x] = from_y(yd, s_yd)
    to_x(xd, s_xd)
    for g in range(tc - 1):
        ring_pass(1, g)

    marks = from_x(xm, s_xm)
    count = marks
    step = 1
    while step < rows * tr:
        count += jnp.where(lane >= step, pltpu.roll(count, step, 1), 0)
        step *= 2
    before = count - marks
    ids = jnp.zeros((SUBLANES, LANES), jnp.int32)
    for s in range(KEEP):
        hit = jnp.logical_and(marks == 1, before == s)
        ids = jnp.where(lane == s, jnp.sum(jnp.where(hit, lane, 0), axis=1, keepdims=True), ids)
    table[...] = ids
    fetch = pltpu.make_async_copy(table, slots, s_local.at[1])
    fetch.start()
    inverse = 1.0 / jnp.where(line < tc, from_x(xd, s_xd), 1.0)
    for q in range(tc):
        inv[c * tc + q] = inverse[q : q + 1]
    for k in near[1:]:
        other = wrap(y + k, ny)
        copy(stage.at[other], stage.at[other], s_stage, k, other, *at_y(k)).wait_recv()
    fetch.wait()

    me = x * tr + h
    for n, (dx, dh) in enumerate(owners):
        s = wrap(x + dx, nx) * tr + wrap(h + dh, tr)
        tile = stage[lax.div(slots[column, s], nx * tr)]
        if n == 0:
            cand[me] = tile
        else:
            cand_out[n] = tile
    order = sorted(range(1, len(owners)), key=lambda n: -min(owners[n][0], nx - owners[n][0]))
    for n in order:
        send(cand_out.at[n], cand.at[me], s_cand, n, me, *at_owner(*owners[n]))
    for k in range(1, cols):
        mine = inv.at[pl.ds(c * tc, tc)]
        send(mine, mine, s_inv, k, c, *at_col(k))

    ring_pass(1, tc - 1)
    for g in range(tc - 1):
        ring_pass(2, g)

    for n in order:
        dx, dh = owners[n]
        other = wrap(x + dx, nx) * tr + wrap(h + dh, tr)
        copy(cand.at[other], cand.at[other], s_cand, n, other, *at_owner(dx, dh)).wait_recv()
    right[slot(x, y)] = cand[lax.rem(slots[column, me], nx * tr)]

    beside = (1, ny - 1)
    spread = sorted(near[1:], key=lambda k: (k in beside, min(k, ny - k)))
    mine = right.at[slot(x, y)]

    def to_others(k):
        part = right.at[slot(x, wrap(y + k, ny))]
        for j in (2, 1, 3):
            send(part, part, s_gx, j * ny + k, j * ny + k, *at_x(j))

    def from_others(k):
        for j in range(1, nx):
            part = right.at[slot(wrap(x - j, nx), wrap(y + k, ny))]
            copy(part, part, s_gx, j * ny + k, j * ny + k, *at_x(-j)).wait_recv()

    to_others(0)
    for k in spread:
        send(mine, mine, s_gy, k, y, *at_y(k))
    ring_pass(2, tc - 1)
    ring_pass(3, 0)
    for n, k in enumerate(spread):
        other = wrap(y + k, ny)
        part = right.at[slot(x, other)]
        copy(part, part, s_gy, k, other, *at_y(k)).wait_recv()
        if k not in beside:
            to_others(k)
        if n == 1:
            from_others(0)
            for j in range(1, nx):
                part = right.at[slot(wrap(x - j, nx), y)]
                for way, to in enumerate((1, -1)):
                    send(part, part, s_next, j * 2 + way, j * 2 + way, *at_y(to))
        if n in (0, 2, 4):
            ring_pass(3, n // 2 + 1)

    for hop in range(4, nz // 2 + 1):
        for g in range(tc):
            ring_pass(hop, g)
    for away in range(nz):
        for g in range(tc):
            pair_wait(away, g)
    for k in range(1, cols):
        other = wrap(c + k, cols)
        part = inv.at[pl.ds(other * tc, tc)]
        copy(part, part, s_inv, k, other, *at_col(k)).wait_recv()
    for q in range(tc):
        for s in range(KEEP):
            tile_row = slots[q, s]
            panel = left[tile_row].reshape(tr * size, size).astype(jnp.float32)
            wide[q, :, s * size : (s + 1) * size] = (panel * inv[tile_row]).astype(jnp.bfloat16)

    for k in range(1, nx):
        for way, to in enumerate((1, -1)):
            part = right.at[slot(wrap(x - k, nx), wrap(y - to, ny))]
            copy(part, part, s_next, k * 2 + way, k * 2 + way, *at_y(-to)).wait_recv()
    for k in spread:
        if k not in beside:
            from_others(k)

    mass = jnp.zeros((SUBLANES, LANES), jnp.float32)
    for q in range(tc):
        tiles = right[q * KEEP : (q + 1) * KEEP].reshape(KEEP * size, size)
        expanded = jnp.dot(wide[q], tiles, preferred_element_type=jnp.float32)
        expanded = expanded * inv[c * tc + q]
        square = expanded * expanded
        out_ref[:, q * size : (q + 1) * size] = square
        mass = jnp.where(line == q, jnp.sum(square, axis=0, keepdims=True), mass)
    rs[r] = mass[:tc]
    for n, (dx, dy) in enumerate(others):
        send(rs.at[r], rs.at[r], s_rs, n, n, *at_row(dx, dy))
    for made in sends:
        made.wait_send()
    for n, (dx, dy) in enumerate(others):
        other, col = at_row(nx - dx, ny - dy)
        copy(rs.at[other], rs.at[other], s_rs, n, n, other, col).wait_recv()
    nodes = rows * tr * size
    share = nodes / sum(rs[k] for k in range(rows))
    for q in range(tc):
        scale_ref[:, q * size : (q + 1) * size] = share[q : q + 1]


def on_device(weights, tile_mask):
    rows, cols = lax.axis_size("row"), lax.axis_size("col")
    tr, tc = tile_mask.shape
    height, width = weights.shape
    size = height // tr
    nx, ny, nz = CHIPS_X, rows // CHIPS_X, cols // CORES
    tiles = tc * cols
    f32, bf16, i32 = jnp.float32, jnp.bfloat16, jnp.int32
    vmem = pltpu.VMEM
    small = (SUBLANES, LANES)

    def pairs(n):
        return pltpu.SemaphoreType.DMA((2, n))

    inflated, scale = pl.pallas_call(
        functools.partial(kernel, size, rows, cols),
        out_shape=(
            jax.ShapeDtypeStruct((height, width), f32),
            jax.ShapeDtypeStruct((1, width), f32),
        ),
        in_specs=[
            pl.BlockSpec(memory_space=pltpu.HBM),
            pl.BlockSpec(memory_space=pltpu.HBM),
        ],
        out_specs=(
            pl.BlockSpec(memory_space=vmem),
            pl.BlockSpec(memory_space=vmem),
        ),
        scratch_shapes=[
            pltpu.SMEM((tr, tc), i32),
            vmem((height, width), bf16),
            vmem((tiles, tr, size, size), bf16),
            vmem((ny, size, size), bf16),
            vmem((ny, size, size), bf16),
            vmem((ny, size, size), bf16),
            vmem((tc * KEEP, size, size), bf16),
            vmem((tc, height, KEEP * size), bf16),
            vmem((nx, *small), i32),
            vmem((nx, *small), f32),
            vmem((ny, *small), i32),
            vmem((ny, *small), f32),
            vmem((rows, tc, size), f32),
            vmem((tiles, 1, size), f32),
            vmem(small, i32),
            pltpu.SMEM(small, i32),
            pairs(nx), pairs(nx), pairs(ny), pairs(ny), pairs(rows),
            pairs(cols), pairs(ny), pairs(KEEP), pairs(ny),
            pairs(nx * ny), pairs(2 * nx), pairs(tc * nz // 2), pairs(tc * nz // 2),
            pairs(tc * nz),
            pltpu.SemaphoreType.DMA((2,)),
        ],
        compiler_params=pltpu.CompilerParams(
            collective_id=0, has_side_effects=True, vmem_limit_bytes=32 * 1024 * 1024
        ),
        name="expand",
    )(
        pltpu.with_memory_space_constraint(tile_mask, pltpu.HBM),
        pltpu.with_memory_space_constraint(weights, pltpu.HBM),
    )
    return inflated * scale


def solution(mesh):
    placed = (P("row", "col"), P("row", "col"))
    return jax.shard_map(
        on_device, mesh=mesh, in_specs=placed, out_specs=P("row", "col"), check_vma=False
    )
```
